256 devices in a mesh: leaf: 64 (over z, y, core), hand: 4 (over x).
Axes of the slice: x: 4, y: 4, z: 8, core: 2. Of those that a mesh axis runs over, the one named last changes fastest.
Arguments:
- opp_range: float32 [1024], P('hand'), may hold values from 0.1 to 1
- br_range: float32 [1024], P('hand'), may hold values from 0.001 to 1
- up_weight: bfloat16 [4, 2048, 1024], P(None, 'leaf', 'hand'), may hold values from 0.29882812 to 1
- up_parent: int32 [3, 2048], replicated, may hold values from 0 to 2047
- board_cards: int32 [6144, 5], P('leaf'), may hold values from 0 to 51, as said below
- hand_rank: int32 [6144, 1024], P('leaf'), may hold values from 0 to 7461
- root_parent: int32 [6144], P('leaf'), may hold values from 0 to 2047
- br_actions: int32 [6144], P('leaf'), may hold values from 1 to 8
- opp_actions: int32 [6144, 8], P('leaf'), may hold values from 1 to 8
- leaf_kind: int32 [6144, 8, 8], P('leaf'), may hold values from 0 to 1
- leaf_stake: int32 [6144, 8, 8], P('leaf'), may hold values from 1 to 400
- opp_weight: bfloat16 [6144, 8, 8, 1024], P('leaf', None, None, 'hand'), may hold values from 0.049804688 to 1
Outputs:
- level_values: float32 [4, 2048, 1024], P(None, 'leaf', 'hand')
- root_value: float32 [1024], P('hand')
- best_value: float32 [], replicated
The draws below stay inside these ranges and needn't reach their ends.
Inputs may be any that keep to these rules, and one draw needn't show every extreme that they name: `board_cards`: five different cards for each subtree.
All inputs are finite; a program needn't handle non-finite values.
Results may differ from the reference program's by a relative error of at most 0.0003.
Values may be sent and summed in bfloat16 or wider, within the bound.
A program may use at most 128 MiB of HBM per device.

```python
import math
import jax
import jax.numpy as jnp
import numpy as np
from jax import lax

HANDS = 1024
ACT = 8
UP = 4
UNODES = 2048
SUBTREES = 6144


def pick_cards(subkey):
    return jax.random.permutation(subkey, 52)[:5]


def draw_board_cards(key, part):
    subkeys = jax.random.split(jax.random.fold_in(key, 17), SUBTREES)
    return jax.vmap(pick_cards)(subkeys).astype(jnp.int32)


def set_ends(values, stream_key, least, high):
    shape = values.shape
    index_at = [jax.random.randint(jax.random.fold_in(stream_key, axis), (), 0, shape[axis]) for axis in range(len(shape))]
    values = values.at[tuple(index_at)].set(least)
    longest = shape.index(max(shape))
    index_at[longest] = (index_at[longest] + 1) % shape[longest]
    return values.at[tuple(index_at)].set(high)


def block_scale(key, extent, pieces, least, high):
    level, own = 1.0, jax.random.fold_in(key, 6)
    for dim, parts in pieces:
        steps = jnp.exp(jax.random.uniform(jax.random.fold_in(own, dim), (parts,), jnp.float32, least / len(pieces), high / len(pieces)))
        level = level * jnp.repeat(steps, extent[dim] // parts).reshape([-1 if axis == dim else 1 for axis in range(len(extent))])
    return level


def setup_inputs(seed: int = 0) -> dict:
    arg_keys = jax.random.split(jax.random.key(seed), 13)
    return {
        "opp_range": jnp.clip(jnp.exp(math.log(1.0) - 2.3025851 * jax.random.uniform(arg_keys[0], (HANDS,), jnp.float32) ** block_scale(arg_keys[0], (HANDS,), ((0, 4),), -0.2, 0.2)), 0.1, 1.0),
        "br_range": jnp.clip(jnp.exp(math.log(1.0) - 6.9077552 * jax.random.uniform(arg_keys[1], (HANDS,), jnp.float32) ** block_scale(arg_keys[1], (HANDS,), ((0, 4),), -0.2, 0.2)), 0.001, 1.0),
        "up_weight": jnp.clip(jnp.exp(math.log(1.0) - 1.2078867 * jax.random.uniform(arg_keys[2], (UP, UNODES, HANDS), jnp.float32) ** block_scale(arg_keys[2], (UP, UNODES, HANDS), ((1, 64), (2, 4)), -0.2, 0.2)), 0.29882812, 1.0).astype(jnp.bfloat16),
        "up_parent": set_ends(jax.random.randint(arg_keys[3], (UP - 1, UNODES), 0, UNODES), jax.random.fold_in(arg_keys[3], 1), 0, UNODES - 1).astype(jnp.int32),
        "board_cards": draw_board_cards(jax.random.fold_in(arg_keys[12], 71), 0),
        "hand_rank": set_ends(jax.random.randint(arg_keys[5], (SUBTREES, HANDS), 0, 7462), jax.random.fold_in(arg_keys[5], 1), 0, 7461).astype(jnp.int32),
        "root_parent": set_ends(jax.random.randint(arg_keys[6], (SUBTREES,), 0, UNODES), jax.random.fold_in(arg_keys[6], 1), 0, UNODES - 1).astype(jnp.int32),
        "br_actions": set_ends(jax.random.randint(arg_keys[7], (SUBTREES,), 1, ACT + 1), jax.random.fold_in(arg_keys[7], 1), 1, ACT).astype(jnp.int32),
        "opp_actions": set_ends(jax.random.randint(arg_keys[8], (SUBTREES, ACT), 1, ACT + 1), jax.random.fold_in(arg_keys[8], 1), 1, ACT).astype(jnp.int32),
        "leaf_kind": set_ends(jax.random.randint(arg_keys[9], (SUBTREES, ACT, ACT), 0, 2), jax.random.fold_in(arg_keys[9], 1), 0, 1).astype(jnp.int32),
        "leaf_stake": set_ends(jax.random.randint(arg_keys[10], (SUBTREES, ACT, ACT), 1, 401), jax.random.fold_in(arg_keys[10], 1), 1, 400).astype(jnp.int32),
        "opp_weight": jnp.clip(jnp.exp(math.log(1.0) - 2.9996462 * jax.random.uniform(arg_keys[11], (SUBTREES, ACT, ACT, HANDS), jnp.float32) ** block_scale(arg_keys[11], (SUBTREES, ACT, ACT, HANDS), ((0, 64), (3, 4)), -0.2, 0.2)), 0.049804688, 1.0).astype(jnp.bfloat16),
    }


PAYOFF_UNIT = 1.0 / 4096.0


def hand_cards(number):
    low_list = []
    high_list = []
    for low_card in range(52):
        for high_card in range(low_card + 1, 52):
            low_list.append(low_card)
            high_list.append(high_card)
    chosen = (np.arange(number) * 1326) // number
    return np.array(low_list, np.int32)[chosen], np.array(high_list, np.int32)[chosen]


def no_shared(low_rows, high_rows, low_cols, high_cols):
    apart_mask = (low_rows[:, None] != low_cols[None, :]) & (low_rows[:, None] != high_cols[None, :])
    apart_mask = apart_mask & (high_rows[:, None] != low_cols[None, :]) & (high_rows[:, None] != high_cols[None, :])
    return apart_mask.astype(jnp.float32)


def board_compat(board_cards, low_cols, high_cols):
    hits = (board_cards[:, :, None] == low_cols[None, None, :]) | (board_cards[:, :, None] == high_cols[None, None, :])
    return 1.0 - jnp.any(hits, axis=1).astype(jnp.float32)


def board_values(packed, noshare):
    root_row, compat_row, rank_row, opp_count, br_count, kind_rows, stake_rows, weight_rows = packed
    legal_mask = (jnp.arange(ACT)[None, :] < opp_count[:, None]).astype(jnp.float32)
    weighted = weight_rows.astype(jnp.float32) * legal_mask[:, :, None]
    probability = weighted / jnp.sum(weighted, axis=1, keepdims=True)
    leaf_reach = (root_row[None, None, :] * probability).astype(jnp.bfloat16).reshape(ACT * ACT, HANDS)
    reach_wide = leaf_reach.astype(jnp.float32)
    order_sign = jnp.sign(rank_row[None, :] - rank_row[:, None]).astype(jnp.float32) * noshare
    showdown = jnp.dot(reach_wide, order_sign, precision=lax.Precision.HIGHEST)
    folded = jnp.dot(reach_wide, noshare, precision=lax.Precision.HIGHEST)
    stake_scaled = stake_rows.reshape(-1).astype(jnp.float32) * PAYOFF_UNIT
    payoff = jnp.where(kind_rows.reshape(-1)[:, None] == 1, showdown, folded) * stake_scaled[:, None] * compat_row[None, :]
    per_node = jnp.sum(payoff.reshape(ACT, ACT, HANDS), axis=1)
    allowed = jnp.arange(ACT)[:, None] < br_count
    return jnp.max(jnp.where(allowed, per_node, -1e30), axis=0)


def reference(opp_range, br_range, up_weight, up_parent, board_cards, hand_rank, root_parent, br_actions, opp_actions, leaf_kind, leaf_stake, opp_weight):
    low_np, high_np = hand_cards(HANDS)
    low_all = jnp.asarray(low_np)
    high_all = jnp.asarray(high_np)
    compat = board_compat(board_cards, low_all, high_all)
    noshare = no_shared(low_all, high_all, low_all, high_all)
    reach_now = opp_range[None, :] * up_weight[0].astype(jnp.float32)
    for level_id in range(1, UP):
        reach_now = jnp.take(reach_now, up_parent[level_id - 1], axis=0) * up_weight[level_id].astype(jnp.float32)
    root_reach = jnp.take(reach_now, root_parent, axis=0) * compat

    def one_board(packed):
        return board_values(packed, noshare)

    sub_value = lax.map(one_board, (root_reach, compat, hand_rank, opp_actions, br_actions, leaf_kind, leaf_stake, opp_weight))
    level_sum = jax.ops.segment_sum(sub_value, root_parent, num_segments=UNODES)
    level_list = [level_sum]
    for level_id in range(UP - 1, 0, -1):
        level_sum = jax.ops.segment_sum(level_sum, up_parent[level_id - 1], num_segments=UNODES)
        level_list.insert(0, level_sum)
    level_values = jnp.stack(level_list)
    root_value = jnp.sum(level_values[0], axis=0) / UNODES
    best_value = jnp.sum(br_range * root_value) / jnp.sum(br_range)
    return level_values, root_value, best_value
```

```python
import functools

import jax
import jax.numpy as jnp
import numpy as np
from jax import lax
from jax.experimental import pallas as pl
from jax.experimental.pallas import tpu as pltpu
from jax.sharding import PartitionSpec as P

MESH = pl.DeviceIdType.MESH
F32 = jnp.float32
BF16 = jnp.bfloat16
PAYOFF_UNIT = 1.0 / 4096.0
VMEM = pltpu.VMEM


def vmem_specs(number):
    return [pl.BlockSpec(memory_space=VMEM)] * number


def exchange_kernel(axis, n, x_ref, o_ref, send_sem, recv_sem, own_sem):
    me = lax.axis_index(axis)
    barrier = pltpu.get_barrier_semaphore()

    def greet(i, carry):
        pl.semaphore_signal(
            barrier, inc=1, device_id={axis: lax.rem(me + i, n)}, device_id_type=MESH
        )
        return carry

    lax.fori_loop(1, n, greet, 0)
    own = pltpu.make_async_copy(x_ref.at[me], o_ref.at[me], own_sem)
    own.start()
    pl.semaphore_wait(barrier, n - 1)

    def send(i, carry):
        peer = lax.rem(me + i, n)
        pltpu.make_async_remote_copy(
            src_ref=x_ref.at[peer],
            dst_ref=o_ref.at[me],
            send_sem=send_sem,
            recv_sem=recv_sem,
            device_id={axis: peer},
            device_id_type=MESH,
        ).start()
        return carry

    lax.fori_loop(1, n, send, 0)
    own.wait()
    others = pl.ds(0, n - 1)
    pltpu.make_async_copy(o_ref.at[others], o_ref.at[others], recv_sem).wait()
    pltpu.make_async_copy(x_ref.at[others], x_ref.at[others], send_sem).wait()


def exchange(x, axis, cid):
    n = x.shape[0]
    return pl.pallas_call(
        functools.partial(exchange_kernel, axis, n),
        out_shape=jax.ShapeDtypeStruct(x.shape, x.dtype),
        in_specs=vmem_specs(1),
        out_specs=pl.BlockSpec(memory_space=VMEM),
        scratch_shapes=[pltpu.SemaphoreType.DMA] * 3,
        compiler_params=pltpu.CompilerParams(collective_id=cid, has_side_effects=True),
        name=f"exchange_{cid}",
    )(x)


def lane_take(table, lanes):
    return jnp.take_along_axis(table, lanes, axis=1, mode="promise_in_bounds")


def look_up(first, second, index):
    lanes = index & 127
    tile = index >> 7
    out = jnp.zeros(index.shape, F32)
    for m in range(8):
        out = jnp.where(tile == m, lane_take(first[m], lanes), out)
        out = jnp.where(tile == m + 8, lane_take(second[m], lanes), out)
    return out


def reach_kernel(w_ref, parent_ref, opp_ref, root_ref, out_ref, now_ref):
    low_half = lax.broadcasted_iota(jnp.int32, (8, 128), 0) < 4

    def tables():
        first, second = [], []
        for m in range(8):
            here = now_ref[:, m * 128 : (m + 1) * 128]
            swapped = pltpu.roll(here, 4, 0)
            first.append(jnp.where(low_half, here, swapped))
            second.append(jnp.where(low_half, swapped, here))
        return first, second

    for m in range(8):
        cut = slice(m * 128, (m + 1) * 128)
        now_ref[:, cut] = w_ref[0, :, cut] * opp_ref[...]
    for level in range(1, 4):
        first, second = tables()
        for m in range(8):
            cut = slice(m * 128, (m + 1) * 128)
            now_ref[:, cut] = (
                look_up(first, second, parent_ref[level - 1, :, cut]) * w_ref[level, :, cut]
            )
    first, second = tables()

    def one(i, carry):
        out_ref[i] = look_up(first, second, root_ref[i])
        return carry

    lax.fori_loop(0, root_ref.shape[0], one, 0)


def leaf_kernel(w_ref, root_ref, flat_ref, out_ref):
    rows, act2, hands = w_ref.shape
    act = act2 // 8
    own_block = lax.broadcasted_iota(jnp.int32, (act, act2), 1) // act == lax.broadcasted_iota(
        jnp.int32, (act, act2), 0
    )
    for s in range(rows):
        flats = flat_ref[s]
        spread = [
            jnp.where(own_block, jnp.broadcast_to(flats[i : i + 1], (act, act2)), 0.0)
            for i in range(5)
        ]
        coef = jnp.concatenate(spread[:4], axis=0).astype(BF16)
        w = w_ref[s]
        total = jnp.dot(spread[4].astype(BF16), w, preferred_element_type=F32)
        factor = root_ref[s : s + 1, :] / total
        wide = w.astype(F32).reshape(act, act, hands) * factor[:, None, :]
        reach = wide.reshape(act2, hands).astype(BF16)
        y = jnp.dot(coef, reach, preferred_element_type=F32)
        y1 = y[0:8] + y[8:16]
        y0 = y[16:24] + y[24:32]
        high1 = y1.astype(BF16).astype(F32)
        high0 = y0.astype(BF16).astype(F32)
        out_ref[s, 0:16, :] = jnp.concatenate([high1, y1 - high1], axis=0).astype(BF16)
        out_ref[s, 16:32, :] = jnp.concatenate([high0, y0 - high0], axis=0).astype(BF16)


def board_kernel(
    br_ref, y_ref, row_ref, col_ref, compat_ref, card_row_ref, card_col_ref, out_ref, apart, minus, sign
):
    group = pl.program_id(0)
    parts, _, _, depth = y_ref.shape
    hands = row_ref.shape[1]

    @pl.when(group == 0)
    def _():
        low_r, high_r = card_row_ref[0:1, :], card_row_ref[1:2, :]

        def strip(i, carry):
            rows = pl.ds(pl.multiple_of(i * 16, 16), 16)
            low_c = jnp.broadcast_to(card_col_ref[rows, 0:1], (16, hands))
            high_c = jnp.broadcast_to(card_col_ref[rows, 1:2], (16, hands))
            share = (low_c == low_r) | (low_c == high_r) | (high_c == low_r) | (high_c == high_r)
            keep = jnp.where(share, 0.0, 1.0)
            apart[rows, :] = keep.astype(BF16)
            minus[rows, :] = (0.0 - keep).astype(BF16)
            return carry

        lax.fori_loop(0, hands // 16, strip, 0)

    folded = jnp.zeros((128, hands), F32)
    for q in range(parts):
        low_rows = y_ref[q, :, 16:32, :].reshape(128, depth)
        folded += jnp.dot(
            low_rows, apart[q * depth : (q + 1) * depth, :], preferred_element_type=F32
        )
    act_row = lax.broadcasted_iota(jnp.int32, (8, hands), 0)
    for s in range(8):
        total = jnp.zeros((16, hands), F32)
        mine = row_ref[s : s + 1, :]
        for q in range(parts):
            slot = (s * parts + q) % 2
            for strip in range(depth // 16):
                at = q * depth + strip * 16
                gap = mine - col_ref[0, at : at + 16, s : s + 1]
                near = gap.astype(BF16)
                sign[slot, strip * 16 : strip * 16 + 16, :] = jnp.maximum(
                    jnp.minimum(near, apart[at : at + 16, :]), minus[at : at + 16, :]
                )
            total += jnp.dot(y_ref[q, s, 0:16, :], sign[slot], preferred_element_type=F32)
        node = total[0:8] + total[8:16] + folded[s * 16 : s * 16 + 8] + folded[s * 16 + 8 : s * 16 + 16]
        node = node * PAYOFF_UNIT * compat_ref[s : s + 1, :]
        node = jnp.where(act_row < br_ref[group * 8 + s], node, -1e30)
        out_ref[s : s + 1, :] = jnp.max(node, axis=0, keepdims=True)


def sums_kernel(v_ref, root_ref, parent_ref, out_ref, total_ref, now_ref):
    sub_row = lax.broadcasted_iota(jnp.int32, (8, 128), 0)
    upper = sub_row // 4
    lane_row = lax.broadcasted_iota(jnp.int32, (128, 128), 0)

    def block(values, index, acc):
        twice = jnp.concatenate([values, values], axis=0)
        high = twice.astype(BF16).astype(F32)
        low = twice - high
        big = jnp.broadcast_to(index >> 7, (8, 128))
        picked_high = [jnp.where(big == 2 * i + upper, high, 0.0) for i in range(8)]
        picked_low = [jnp.where(big == 2 * i + upper, low, 0.0) for i in range(8)]
        left = jnp.concatenate(picked_high + picked_low, axis=0).astype(BF16)
        right = jnp.where(jnp.broadcast_to(index & 127, (128, 128)) == lane_row, 1.0, 0.0).astype(BF16)
        return acc + lax.dot_general(
            left, right, (((1,), (1,)), ((), ())), preferred_element_type=F32
        )

    def from_boards(i, acc):
        return block(v_ref[i], root_ref[pl.ds(i, 1), :], acc)

    acc = lax.fori_loop(0, v_ref.shape[0], from_boards, jnp.zeros((128, 128), F32))
    levels = [None] * 4
    for level in range(3, -1, -1):
        levels[level] = acc[0:64] + acc[64:128]
        if level > 0:
            acc = jnp.zeros((128, 128), F32)
            for t in range(16):
                acc = block(
                    levels[level][4 * t : 4 * t + 4], parent_ref[level - 1, t : t + 1, :], acc
                )
    place = lax.broadcasted_iota(jnp.int32, (64, 128), 1) // 32
    for q in range(4):
        out = jnp.zeros((64, 128), F32)
        for level in range(4):
            shift = ((level - q) * 32) % 128
            moved = levels[level] if shift == 0 else pltpu.roll(levels[level], shift, 1)
            out = jnp.where(place == level, moved, out)
        out_ref[q] = out
    total_ref[...] = levels[0]


def hand_cards(number):
    low_list = []
    high_list = []
    for low_card in range(52):
        for high_card in range(low_card + 1, 52):
            low_list.append(low_card)
            high_list.append(high_card)
    chosen = np.arange(number) * 1326 // number
    return (np.array(low_list, np.int32)[chosen], np.array(high_list, np.int32)[chosen])


def board_compat(board_cards, low_cols, high_cols):
    hits = (board_cards[:, :, None] == low_cols[None, None, :]) | (
        board_cards[:, :, None] == high_cols[None, None, :]
    )
    return 1.0 - jnp.any(hits, axis=1).astype(F32)


def local(
    opp_range,
    br_range,
    up_weight,
    up_parent,
    board_cards,
    hand_rank,
    root_parent,
    br_actions,
    opp_actions,
    leaf_kind,
    leaf_stake,
    opp_weight,
):
    leaf_at = lax.axis_index("leaf")
    hand_at = lax.axis_index("hand")
    low_np, high_np = hand_cards(1024)
    low_all, high_all = jnp.asarray(low_np), jnp.asarray(high_np)
    low_mine = lax.dynamic_slice_in_dim(low_all, hand_at * 256, 256)
    high_mine = lax.dynamic_slice_in_dim(high_all, hand_at * 256, 256)

    out1 = up_weight.astype(F32).reshape(128, 256).T.reshape(64, 4, 128)
    parents = jnp.pad(root_parent.astype(F32), (0, 32))
    out1 = jnp.concatenate([out1, jnp.broadcast_to(parents, (64, 1, 128))], axis=1)
    got1 = exchange(out1, "leaf", 0)
    weights = got1[:, :4].reshape(32 * 2, 4, 4, 32).transpose(2, 1, 0, 3).reshape(4, 4, 2, 1024)
    weights = weights.transpose(0, 2, 1, 3).reshape(4, 8, 1024)
    roots = got1[:, 4].astype(jnp.int32)
    root_index = jnp.broadcast_to(roots[:, None, :], (64, 4, 128)).reshape(32, 8, 128)
    parent_index = jnp.broadcast_to(up_parent.reshape(3, 2, 1, 1024), (3, 2, 4, 1024)).reshape(3, 8, 1024)
    opp4 = lax.dynamic_slice_in_dim(opp_range, leaf_at * 4, 4)
    opp8 = jnp.broadcast_to(jnp.concatenate([opp4, opp4])[:, None], (8, 128))
    out2 = pl.pallas_call(
        reach_kernel,
        out_shape=jax.ShapeDtypeStruct((32, 8, 128), F32),
        in_specs=vmem_specs(4),
        out_specs=pl.BlockSpec(memory_space=VMEM),
        scratch_shapes=[VMEM((8, 1024), F32)],
        name="reach",
    )(weights, parent_index, opp8, root_index)
    got2 = exchange(out2.reshape(64, 4, 128), "leaf", 1)
    compat = board_compat(board_cards, low_mine, high_mine)
    root_reach = got2.reshape(256, 128).T[:96] * compat

    legal = (jnp.arange(8)[None, None, :] < opp_actions[:, :, None]).astype(jnp.int32)
    shown = (leaf_kind == 1).astype(jnp.int32) * leaf_stake * legal
    fold = (leaf_kind != 1).astype(jnp.int32) * leaf_stake * legal
    flats = jnp.stack(
        [shown & ~15, shown & 15, fold & ~15, fold & 15, legal, legal, legal, legal], axis=1
    )
    flats = flats.reshape(96, 8, 64).astype(F32)
    weights_flat = opp_weight.reshape(96, 64, 256)
    y = pl.pallas_call(
        leaf_kernel,
        grid=(12,),
        out_shape=jax.ShapeDtypeStruct((96, 32, 256), BF16),
        in_specs=[
            pl.BlockSpec((8, 64, 256), lambda i: (i, 0, 0)),
            pl.BlockSpec((8, 256), lambda i: (i, 0)),
            pl.BlockSpec((8, 8, 64), lambda i: (i, 0, 0)),
        ],
        out_specs=pl.BlockSpec((8, 32, 256), lambda i: (i, 0, 0)),
        name="leaf",
    )(weights_flat, root_reach, flats)
    y_all = exchange(y.reshape(4, 24, 32, 256), "hand", 2)

    ranks = lax.dynamic_slice_in_dim(hand_rank, hand_at * 24, 24).astype(F32)
    boards = lax.dynamic_slice_in_dim(board_cards, hand_at * 24, 24)
    br_mine = lax.dynamic_slice_in_dim(br_actions, hand_at * 24, 24)
    compat_all = board_compat(boards, low_all, high_all)
    columns = ranks.reshape(3, 8, 1024).transpose(0, 2, 1)
    cards = jnp.stack([low_all, high_all]).astype(F32)
    sub = pl.pallas_call(
        board_kernel,
        grid_spec=pltpu.PrefetchScalarGridSpec(
            num_scalar_prefetch=1,
            grid=(3,),
            in_specs=[
                pl.BlockSpec((4, 8, 32, 256), lambda i, br: (0, i, 0, 0)),
                pl.BlockSpec((8, 1024), lambda i, br: (i, 0)),
                pl.BlockSpec((1, 1024, 8), lambda i, br: (i, 0, 0)),
                pl.BlockSpec((8, 1024), lambda i, br: (i, 0)),
                pl.BlockSpec((2, 1024), lambda i, br: (0, 0)),
                pl.BlockSpec((1024, 2), lambda i, br: (0, 0)),
            ],
            out_specs=pl.BlockSpec((8, 1024), lambda i, br: (i, 0)),
            scratch_shapes=[
                VMEM((1024, 1024), BF16),
                VMEM((1024, 1024), BF16),
                VMEM((2, 256, 1024), BF16),
            ],
        ),
        out_shape=jax.ShapeDtypeStruct((24, 1024), F32),
        name="boards",
    )(br_mine, y_all, ranks, columns, compat_all, cards, cards.T)
    sub_value = exchange(sub.reshape(24, 4, 256).transpose(1, 0, 2), "hand", 3).reshape(96, 256)

    out3 = jnp.pad(sub_value.T, ((0, 0), (0, 32))).reshape(64, 4, 128)
    got3 = exchange(out3, "leaf", 4)
    level_out, totals = pl.pallas_call(
        sums_kernel,
        out_shape=(
            jax.ShapeDtypeStruct((4, 64, 128), F32),
            jax.ShapeDtypeStruct((64, 128), F32),
        ),
        in_specs=vmem_specs(3),
        out_specs=(pl.BlockSpec(memory_space=VMEM), pl.BlockSpec(memory_space=VMEM)),
        scratch_shapes=[VMEM((8, 128), F32)],
        name="sums",
    )(got3, roots, up_parent.reshape(3, 16, 128))
    root4 = jnp.sum(totals.reshape(16, 4, 128), axis=(0, 2))
    out4 = level_out.reshape(4, 16, 4, 128).transpose(1, 0, 2, 3).reshape(64, 4, 128)
    root_row = jnp.broadcast_to(jnp.pad(root4, (0, 124)), (64, 1, 128))
    got4 = exchange(jnp.concatenate([out4, root_row], axis=1), "leaf", 5)
    level_values = got4[:, :4].reshape(256, 128).T.reshape(4, 32, 256)
    root_value = got4[:, 4, :4].reshape(256) / 2048
    pair = jnp.stack([jnp.sum(br_range * root_value), jnp.sum(br_range)])
    pair = jnp.broadcast_to(jnp.pad(pair, (0, 126)), (4, 8, 128))
    both = exchange(pair, "hand", 6)
    both = jnp.sum(both[:, 0], axis=0)
    return level_values, root_value, both[0] / both[1]


def solution(mesh):
    in_specs = (
        P("hand"),
        P("hand"),
        P(None, "leaf", "hand"),
        P(),
        P("leaf", None),
        P("leaf", None),
        P("leaf"),
        P("leaf"),
        P("leaf", None),
        P("leaf", None, None),
        P("leaf", None, None),
        P("leaf", None, None, "hand"),
    )
    out_specs = (P(None, "leaf", "hand"), P("hand"), P())
    return jax.shard_map(local, mesh=mesh, in_specs=in_specs, out_specs=out_specs, check_vma=False)
```

```python
import jax
import jax.numpy as jnp
import numpy as np
from jax import lax
from jax.experimental import pallas as pl
from jax.experimental.pallas import tpu as pltpu
from jax.sharding import PartitionSpec as P

MESH = pl.DeviceIdType.MESH
F32 = jnp.float32
BF16 = jnp.bfloat16
I32 = jnp.int32
PAYOFF_UNIT = 1.0 / 4096.0
VMEM = pltpu.VMEM
LEAVES = 64
SIDES = 4


def dot(a, b):
    return jnp.dot(a, b, preferred_element_type=F32)


def dot_t(a, b):
    return lax.dot_general(a, b, (((1,), (1,)), ((), ())), preferred_element_type=F32)


def lane_take(table, lanes):
    return jnp.take_along_axis(table, lanes, axis=1, mode="promise_in_bounds")


def look_up(first, second, index):
    lanes = index & 127
    tile = index >> 7
    parts = []
    for m in range(8):
        parts.append(jnp.where(tile == m, lane_take(first[m], lanes), 0.0))
        parts.append(jnp.where(tile == m + 8, lane_take(second[m], lanes), 0.0))
    while len(parts) > 1:
        parts = [parts[i] + parts[i + 1] for i in range(0, len(parts), 2)]
    return parts[0]


def card_hits(card, low, high):
    return (card == low) | (card == high)


def kernel(
    br_act,
    up_ref,
    root_ref,
    parent_ref,
    opp_ref,
    br_ref,
    cards_ref,
    card_col_ref,
    board_ref,
    rank_ref,
    code_ref,
    w_hbm,
    level_ref,
    value_ref,
    best_ref,
    w_ref,
    apart,
    minus,
    sign,
    s1,
    r1,
    s2,
    r2,
    s3,
    r3,
    s4,
    r4,
    sy,
    ry,
    sx,
    rx,
    br_all,
    weights,
    now_ref,
    turned,
    board_sum,
    reach_ref,
    inverse,
    column,
    node_ref,
    compat_all,
    sub_ref,
    left,
    right,
    right_up,
    leaf_send,
    leaf_recv,
    own_sem,
    w_sem,
    y_send,
    y_recv,
    x_send,
    x_recv,
    b_send,
    b_recv,
):
    leaf_at = lax.axis_index("leaf")
    hand_at = lax.axis_index("hand")
    barrier = pltpu.get_barrier_semaphore()

    def greet_leaf(i, carry):
        pl.semaphore_signal(
            barrier, inc=1, device_id={"leaf": lax.rem(leaf_at + i, LEAVES)}, device_id_type=MESH
        )
        return carry

    lax.fori_loop(1, LEAVES, greet_leaf, 0)
    for i in range(1, SIDES):
        pl.semaphore_signal(
            barrier, inc=1, device_id={"hand": lax.rem(hand_at + i, SIDES)}, device_id_type=MESH
        )
    w_copy = pltpu.make_async_copy(w_hbm, w_ref, w_sem)
    w_copy.start()

    def leaf_start(number, src, dst):
        own = pltpu.make_async_copy(src.at[leaf_at], dst.at[leaf_at], own_sem.at[number])
        own.start()

        def send(i, carry):
            peer = lax.rem(leaf_at + i, LEAVES)
            pltpu.make_async_remote_copy(
                src_ref=src.at[peer],
                dst_ref=dst.at[leaf_at],
                send_sem=leaf_send.at[number],
                recv_sem=leaf_recv.at[number],
                device_id={"leaf": peer},
                device_id_type=MESH,
            ).start()
            return carry

        lax.fori_loop(1, LEAVES, send, 0)
        return own

    def leaf_wait(number, own, src, dst):
        own.wait()
        others = pl.ds(0, LEAVES - 1)
        pltpu.make_async_copy(dst.at[others], dst.at[others], leaf_recv.at[number]).wait()
        pltpu.make_async_copy(src.at[others], src.at[others], leaf_send.at[number]).wait()

    root_row = jnp.concatenate(
        [root_ref[...].astype(F32), jnp.zeros((1, 32), F32)], axis=1
    )
    for half in range(2):
        turned[half * 128 : half * 128 + 128, :] = (
            up_ref[:, half * 128 : half * 128 + 128].astype(F32).T
        )
    for d in range(LEAVES):
        s1[d, 0:4, :] = turned[4 * d : 4 * d + 4, :]
        s1[d, 4:5, :] = root_row
    pl.semaphore_wait(barrier, LEAVES - 1 + SIDES - 1)
    own1 = leaf_start(0, s1, r1)
    br_copies = []
    for i in range(1, SIDES):
        peer = lax.rem(hand_at + i, SIDES)
        copy = pltpu.make_async_remote_copy(
            src_ref=br_ref,
            dst_ref=br_all.at[hand_at],
            send_sem=b_send.at[i],
            recv_sem=b_recv.at[i],
            device_id={"hand": peer},
            device_id_type=MESH,
        )
        copy.start()
        br_copies.append(copy)
    br_all[hand_at] = br_ref[...]

    low_r, high_r = cards_ref[0:1, :], cards_ref[1:2, :]

    def strip(i, carry):
        rows = pl.ds(pl.multiple_of(i * 16, 16), 16)
        low_c = jnp.broadcast_to(card_col_ref[rows, 0:1], (16, 1024))
        high_c = jnp.broadcast_to(card_col_ref[rows, 1:2], (16, 1024))
        share = card_hits(low_c, low_r, high_r) | card_hits(high_c, low_r, high_r)
        keep = jnp.where(share, 0.0, 1.0)
        apart[rows, :] = keep.astype(BF16)
        minus[rows, :] = (0.0 - keep).astype(BF16)
        return carry

    lax.fori_loop(0, 64, strip, 0)
    for g in range(3):
        rows = pl.ds(pl.multiple_of(hand_at * 24 + g * 8, 8), 8)
        for m in range(8):
            column[g, m * 128 : m * 128 + 128, 0:8] = (
                rank_ref[rows, m * 128 : m * 128 + 128].astype(F32).T
            )
        hit = jnp.zeros((8, 1024), F32)
        for c in range(5):
            card = jnp.broadcast_to(board_ref[rows, c : c + 1], (8, 1024))
            hit = jnp.where(card_hits(card, low_r, high_r), 1.0, hit)
        compat_all[g * 8 : g * 8 + 8, :] = (1.0 - hit) * PAYOFF_UNIT
    lane_row = lax.broadcasted_iota(I32, (128, 128), 0)
    for k in range(3):
        for t in range(16):
            index = parent_ref[k : k + 1, t * 128 : t * 128 + 128] & 127
            right_up[k, :, t * 128 : t * 128 + 128] = jnp.where(
                jnp.broadcast_to(index, (128, 128)) == lane_row, 1.0, 0.0
            ).astype(BF16)

    leaf_wait(0, own1, s1, r1)

    low_half = lax.broadcasted_iota(I32, (8, 128), 0) < 4
    place8 = lax.broadcasted_iota(I32, (8, 128), 1) // 32
    for m in range(8):
        pairs = [
            jnp.concatenate([r1[4 * m + q, 0:4, :], r1[32 + 4 * m + q, 0:4, :]], axis=0)
            for q in range(4)
        ]
        for level in range(4):
            out = jnp.zeros((8, 128), F32)
            for q in range(4):
                shift = ((q - level) * 32) % 128
                moved = pairs[q] if shift == 0 else pltpu.roll(pairs[q], shift, 1)
                out = jnp.where(place8 == q, moved, out)
            if level == 0:
                now_ref[:, m * 128 : m * 128 + 128] = out
            else:
                weights[level - 1, :, m * 128 : m * 128 + 128] = out

    def tables():
        first, second = [], []
        for m in range(8):
            here = now_ref[:, m * 128 : (m + 1) * 128]
            swapped = pltpu.roll(here, 4, 0)
            first.append(jnp.where(low_half, here, swapped))
            second.append(jnp.where(low_half, swapped, here))
        return first, second

    def wide_row(a, b):
        return jnp.where(low_half, jnp.broadcast_to(a, (8, 128)), jnp.broadcast_to(b, (8, 128)))

    for level in range(3):
        first, second = tables()
        for m in range(8):
            cut = slice(m * 128, (m + 1) * 128)
            index = wide_row(
                parent_ref[level : level + 1, m * 128 : m * 128 + 128],
                parent_ref[level : level + 1, 1024 + m * 128 : 1024 + m * 128 + 128],
            )
            now_ref[:, cut] = look_up(first, second, index) * weights[level, :, cut]
    first, second = tables()

    def reach_of(i, carry):
        index = wide_row(r1[2 * i, 4:5, :], r1[2 * i + 1, 4:5, :]).astype(I32)
        out = look_up(first, second, index)
        s2[2 * i] = out[0:4]
        s2[2 * i + 1] = out[4:8]
        return carry

    lax.fori_loop(0, 32, reach_of, 0)
    own2 = leaf_start(1, s2, r2)

    w_copy.wait()
    lane64 = lax.broadcasted_iota(I32, (8, 128), 1)
    own_block = (lane64 // 8 == lax.broadcasted_iota(I32, (8, 128), 0)) & (lane64 < 64)
    inner = lane64 & 7

    def spread_code(s):
        code = jnp.concatenate([code_ref[s], jnp.zeros((8, 120), F32)], axis=1)
        return jnp.where(own_block, lane_take(code, inner), 0.0)[:, 0:64]

    def totals(i, carry):
        for k in range(8):
            s = i * 8 + k
            legal = jnp.where(spread_code(s) == 0.0, 0.0, 1.0).astype(BF16)
            inverse[s] = 1.0 / dot(legal, w_ref[s])
        return carry

    lax.fori_loop(0, 12, totals, 0)

    def target(i, carry):
        index = r1[i, 4:5, :].astype(I32) & 127
        right[i] = jnp.where(
            jnp.broadcast_to(index, (128, 128)) == lane_row, 1.0, 0.0
        ).astype(BF16)
        return carry

    lax.fori_loop(0, LEAVES, target, 0)
    mine = pl.ds(pl.multiple_of(hand_at * 256, 256), 256)
    low_m, high_m = cards_ref[0:1, mine], cards_ref[1:2, mine]
    for g in range(12):
        hit = jnp.zeros((8, 256), F32)
        for c in range(5):
            card = jnp.broadcast_to(board_ref[g * 8 : g * 8 + 8, c : c + 1], (8, 256))
            hit = jnp.where(card_hits(card, low_m, high_m), 1.0, hit)
        board_sum[g * 8 : g * 8 + 8, :] = (1.0 - hit) * opp_ref[...]

    leaf_wait(1, own2, s2, r2)

    for d in range(LEAVES):
        turned[4 * d : 4 * d + 4, :] = r2[d]
    for half in range(2):
        cut = slice(half * 128, half * 128 + 128)
        reach_ref[:, cut] = turned[cut, :].T[0:96, :] * board_sum[0:96, cut]

    def leaf_group(dst, base, g):
        for k in range(8):
            s = base + g * 8 + k
            code = spread_code(s)
            stake = jnp.abs(code)
            high = jnp.floor(stake * 0.0625) * 16.0
            low = stake - high
            shown = code < 0.0
            coef = jnp.concatenate(
                [
                    jnp.where(shown, high, 0.0),
                    jnp.where(shown, low, 0.0),
                    jnp.where(shown, 0.0, high),
                    jnp.where(shown, 0.0, low),
                ],
                axis=0,
            ).astype(BF16)
            factor = reach_ref[pl.ds(s, 1), :] * inverse[s]
            wide = w_ref[s].astype(F32).reshape(8, 8, 256) * factor[:, None, :]
            y = dot(coef, wide.reshape(64, 256).astype(BF16))
            y1 = y[0:8] + y[8:16]
            y0 = y[16:24] + y[24:32]
            high1 = y1.astype(BF16).astype(F32)
            high0 = y0.astype(BF16).astype(F32)
            dst[g * 8 + k, 0:16, :] = jnp.concatenate([high1, y1 - high1], axis=0).astype(BF16)
            dst[g * 8 + k, 16:32, :] = jnp.concatenate([high0, y0 - high0], axis=0).astype(BF16)

    y_copies = []
    for i in (2, 1, 3):
        peer = lax.rem(hand_at + i, SIDES)

        def group_of(g, carry):
            leaf_group(sy.at[peer], peer * 24, g)
            return carry

        lax.fori_loop(0, 3, group_of, 0)
        copy = pltpu.make_async_remote_copy(
            src_ref=sy.at[peer],
            dst_ref=ry.at[hand_at],
            send_sem=y_send.at[i],
            recv_sem=y_recv.at[i],
            device_id={"hand": peer},
            device_id_type=MESH,
        )
        copy.start()
        y_copies.append(copy)

    def group_own(g, carry):
        leaf_group(ry.at[hand_at], hand_at * 24, g)
        return carry

    lax.fori_loop(0, 3, group_own, 0)

    def one_pass(q, first_pass):
        base = q * 256

        def group_of(g, carry):
            rows24 = pl.ds(pl.multiple_of(hand_at * 24 + g * 8, 8), 8)
            ranks = rank_ref[rows24, :].astype(F32)
            lows = ry[q, pl.ds(pl.multiple_of(g * 8, 8), 8), 16:32, :].reshape(128, 256)
            fold = dot(lows, apart[pl.ds(pl.multiple_of(base, 256), 256), :])
            for s in range(8):
                for part in range(16):
                    at = pl.multiple_of(base + part * 16, 16)
                    gap = ranks[s : s + 1] - column[g, pl.ds(at, 16), s : s + 1]
                    sign[s % 2, part * 16 : part * 16 + 16, :] = jnp.maximum(
                        jnp.minimum(gap.astype(BF16), apart[pl.ds(at, 16), :]),
                        minus[pl.ds(at, 16), :],
                    )
                total = dot(ry[q, g * 8 + s, 0:16, :], sign[s % 2])
                node = total[0:8] + total[8:16]
                node = node + (fold[s * 16 : s * 16 + 8] + fold[s * 16 + 8 : s * 16 + 16])
                if not first_pass:
                    node = node + node_ref[g * 8 + s]
                node_ref[g * 8 + s] = node
            return carry

        lax.fori_loop(0, 3, group_of, 0)

    one_pass(hand_at, True)
    for i, copy in zip((1, 3, 2), (y_copies[1], y_copies[2], y_copies[0])):
        copy.wait_recv()
        one_pass(lax.rem(hand_at + SIDES - i, SIDES), False)
    for copy in y_copies:
        copy.wait_send()
    for copy in br_copies:
        copy.wait()

    act_row = lax.broadcasted_iota(I32, (8, 1024), 0)

    def best_of(g, carry):
        for k in range(8):
            s = g * 8 + k
            value = node_ref[s] * compat_all[pl.ds(s, 1), :]
            value = jnp.where(act_row < br_act[hand_at * 24 + s], value, -1e30)
            sub_ref[pl.ds(s, 1), :] = jnp.max(value, axis=0, keepdims=True)
        return carry

    lax.fori_loop(0, 3, best_of, 0)
    board_total = jnp.sum(sub_ref[...], axis=0, keepdims=True)
    weighted = jnp.zeros((1, 256), F32)
    range_sum = jnp.zeros((1, 256), F32)
    for p in range(SIDES):
        weighted += board_total[:, p * 256 : p * 256 + 256] * br_all[p]
        range_sum += br_all[p]
    for p in range(SIDES):
        sx[p, 0:24, :] = sub_ref[:, p * 256 : p * 256 + 256]
        sx[p, 24:25, :] = weighted
    rx[hand_at] = sx[hand_at]
    x_copies = []
    for i in (2, 1, 3):
        peer = lax.rem(hand_at + i, SIDES)
        copy = pltpu.make_async_remote_copy(
            src_ref=sx.at[peer],
            dst_ref=rx.at[hand_at],
            send_sem=x_send.at[i],
            recv_sem=x_recv.at[i],
            device_id={"hand": peer},
            device_id_type=MESH,
        )
        copy.start()
        x_copies.append(copy)
    for copy in x_copies:
        copy.wait()

    for p in range(SIDES):
        board_sum[p * 24 : p * 24 + 24, :] = rx[p, 0:24, :]
    board_sum[96:128, :] = jnp.zeros((32, 256), F32)
    sides = (rx[0, 24:25, :] + rx[1, 24:25, :]) + (rx[2, 24:25, :] + rx[3, 24:25, :])
    side_row = sides[:, 0:128] + sides[:, 128:256]
    for half in range(2):
        cut = slice(half * 128, half * 128 + 128)
        turned[cut, :] = board_sum[:, cut].T
    for d in range(LEAVES):
        s3[d, 0:4, :] = turned[4 * d : 4 * d + 4, :]
        s3[d, 4:5, :] = side_row
    own3 = leaf_start(2, s3, r3)
    leaf_wait(2, own3, s3, r3)

    upper = lax.broadcasted_iota(I32, (8, 128), 0) // 4

    def choose(values, index, put):
        twice = jnp.concatenate([values, values], axis=0)
        high = twice.astype(BF16).astype(F32)
        low = twice - high
        big = jnp.broadcast_to(index >> 7, (8, 128))
        for i in range(4):
            is_a, is_b = big == 4 * i + upper, big == 4 * i + 2 + upper
            put(
                i * 16,
                jnp.concatenate(
                    [jnp.where(is_a, high, 0.0), jnp.where(is_b, high, 0.0)], axis=0
                ).astype(BF16),
            )
            put(
                64 + i * 16,
                jnp.concatenate(
                    [jnp.where(is_a, low, 0.0), jnp.where(is_b, low, 0.0)], axis=0
                ).astype(BF16),
            )

    def from_boards(j, carry):
        for k in range(4):
            i = j * 4 + k

            def put(row, block):
                left[i, row : row + 16, :] = block

            choose(r3[i, 0:4, :], r1[i, 4:5, :].astype(I32), put)
        return carry

    lax.fori_loop(0, 16, from_boards, 0)
    acc = jnp.zeros((128, 128), F32)
    for i in range(0, LEAVES, 2):
        acc = acc + dot_t(
            jnp.concatenate([left[i], left[i + 1]], axis=1),
            jnp.concatenate([right[i], right[i + 1]], axis=1),
        )
    levels = [None] * 4
    levels[3] = acc[0:64] + acc[64:128]
    for level in range(2, -1, -1):
        for t in range(16):

            def put(row, block, t=t):
                left[t, row : row + 16, :] = block

            choose(
                levels[level + 1][4 * t : 4 * t + 4],
                parent_ref[level : level + 1, t * 128 : t * 128 + 128],
                put,
            )
        acc = jnp.zeros((128, 128), F32)
        for t in range(0, 16, 2):
            acc = acc + dot_t(
                jnp.concatenate([left[t], left[t + 1]], axis=1),
                right_up[level, :, t * 128 : t * 128 + 256],
            )
        levels[level] = acc[0:64] + acc[64:128]

    column_sum = jnp.zeros((8, 128), F32)
    for t in range(8):
        column_sum = column_sum + levels[0][8 * t : 8 * t + 8]
    column_sum = column_sum[0:4] + column_sum[4:8]
    root4 = jnp.sum(column_sum, axis=1, keepdims=True) * (1.0 / 2048.0)
    spot = lax.rem(leaf_at, 32) * 4
    lane4 = lax.broadcasted_iota(I32, (4, 128), 1)
    at4 = lane4 == lax.broadcasted_iota(I32, (4, 128), 0) + spot
    placed = jnp.sum(jnp.where(at4, root4, 0.0), axis=0, keepdims=True)
    is_second = jnp.broadcast_to(leaf_at // 32, (1, 128)) == 1
    row_a = jnp.where(is_second, 0.0, placed)
    row_b = jnp.where(is_second, placed, 0.0)
    place64 = lax.broadcasted_iota(I32, (64, 128), 1) // 32
    for q in range(4):
        out = jnp.zeros((64, 128), F32)
        for level in range(4):
            shift = ((level - q) * 32) % 128
            moved = levels[level] if shift == 0 else pltpu.roll(levels[level], shift, 1)
            out = jnp.where(place64 == level, moved, out)
        for t in range(16):
            s4[4 * t + q, 0:4, :] = out[4 * t : 4 * t + 4]
            s4[4 * t + q, 4:5, :] = row_a
            s4[4 * t + q, 5:6, :] = row_b
    own4 = leaf_start(3, s4, r4)
    best_sum = jnp.zeros((1, 128), F32)
    for d in range(LEAVES):
        best_sum = best_sum + r3[d, 4:5, :]
    numerator = jnp.sum(best_sum, axis=1, keepdims=True) * (1.0 / 2048.0)
    denominator = jnp.sum(range_sum, axis=1, keepdims=True)
    best_ref[...] = numerator / denominator
    leaf_wait(3, own4, s4, r4)
    value_a = jnp.zeros((1, 128), F32)
    value_b = jnp.zeros((1, 128), F32)
    for d in range(LEAVES):
        turned[4 * d : 4 * d + 4, :] = r4[d, 0:4, :]
        value_a = value_a + r4[d, 4:5, :]
        value_b = value_b + r4[d, 5:6, :]
    value_ref[:, 0:128] = value_a
    value_ref[:, 128:256] = value_b
    for half in range(2):
        cut = slice(half * 128, half * 128 + 128)
        level_ref[:, cut] = turned[cut, :].T


def hand_cards(number):
    low_list = []
    high_list = []
    for low_card in range(52):
        for high_card in range(low_card + 1, 52):
            low_list.append(low_card)
            high_list.append(high_card)
    chosen = np.arange(number) * 1326 // number
    return np.stack([np.array(low_list)[chosen], np.array(high_list)[chosen]]).astype(np.int32)


def local(
    opp_range,
    br_range,
    up_weight,
    up_parent,
    board_cards,
    hand_rank,
    root_parent,
    br_actions,
    opp_actions,
    leaf_kind,
    leaf_stake,
    opp_weight,
):
    cards = hand_cards(1024)
    legal = jnp.arange(8)[None, None, :] < opp_actions[:, :, None]
    code = jnp.where(legal, jnp.where(leaf_kind == 1, -leaf_stake, leaf_stake), 0).astype(F32)
    vmem = pl.BlockSpec(memory_space=VMEM)
    level_out, root_value, best = pl.pallas_call(
        kernel,
        out_shape=(
            jax.ShapeDtypeStruct((128, 256), F32),
            jax.ShapeDtypeStruct((1, 256), F32),
            jax.ShapeDtypeStruct((1, 1), F32),
        ),
        in_specs=[pl.BlockSpec(memory_space=pltpu.SMEM)]
        + [vmem] * 10
        + [pl.BlockSpec(memory_space=pl.ANY)],
        out_specs=(vmem, vmem, vmem),
        scratch_shapes=[
            VMEM((96, 64, 256), BF16),
            VMEM((1024, 1024), BF16),
            VMEM((1024, 1024), BF16),
            VMEM((2, 256, 1024), BF16),
            VMEM((LEAVES, 5, 128), F32),
            VMEM((LEAVES, 5, 128), F32),
            VMEM((LEAVES, 4, 128), F32),
            VMEM((LEAVES, 4, 128), F32),
            VMEM((LEAVES, 5, 128), F32),
            VMEM((LEAVES, 5, 128), F32),
            VMEM((LEAVES, 6, 128), F32),
            VMEM((LEAVES, 6, 128), F32),
            VMEM((SIDES, 24, 32, 256), BF16),
            VMEM((SIDES, 24, 32, 256), BF16),
            VMEM((SIDES, 25, 256), F32),
            VMEM((SIDES, 25, 256), F32),
            VMEM((SIDES, 1, 256), F32),
            VMEM((3, 8, 1024), F32),
            VMEM((8, 1024), F32),
            VMEM((256, 128), F32),
            VMEM((128, 256), F32),
            VMEM((96, 256), F32),
            VMEM((96, 8, 256), F32),
            VMEM((3, 1024, 8), F32),
            VMEM((24, 8, 1024), F32),
            VMEM((24, 1024), F32),
            VMEM((24, 1024), F32),
            VMEM((LEAVES, 128, 128), BF16),
            VMEM((LEAVES, 128, 128), BF16),
            VMEM((3, 128, 2048), BF16),
            pltpu.SemaphoreType.DMA((4,)),
            pltpu.SemaphoreType.DMA((4,)),
            pltpu.SemaphoreType.DMA((4,)),
            pltpu.SemaphoreType.DMA,
            pltpu.SemaphoreType.DMA((4,)),
            pltpu.SemaphoreType.DMA((4,)),
            pltpu.SemaphoreType.DMA((4,)),
            pltpu.SemaphoreType.DMA((4,)),
            pltpu.SemaphoreType.DMA((4,)),
            pltpu.SemaphoreType.DMA((4,)),
        ],
        compiler_params=pltpu.CompilerParams(collective_id=0, has_side_effects=True),
        name="tree",
    )(
        br_actions,
        up_weight.reshape(128, 256),
        root_parent.reshape(1, 96),
        up_parent,
        opp_range.reshape(1, 256),
        br_range.reshape(1, 256),
        jnp.asarray(cards),
        jnp.asarray(cards.T),
        board_cards,
        hand_rank,
        code,
        opp_weight.reshape(96, 64, 256),
    )
    return level_out.reshape(4, 32, 256), root_value.reshape(256), best[0, 0]


def solution(mesh):
    in_specs = (
        P("hand"),
        P("hand"),
        P(None, "leaf", "hand"),
        P(),
        P("leaf", None),
        P("leaf", None),
        P("leaf"),
        P("leaf"),
        P("leaf", None),
        P("leaf", None, None),
        P("leaf", None, None),
        P("leaf", None, None, "hand"),
    )
    out_specs = (P(None, "leaf", "hand"), P("hand"), P())
    return jax.shard_map(local, mesh=mesh, in_specs=in_specs, out_specs=out_specs, check_vma=False)
```

```python
import jax
import jax.numpy as jnp
import numpy as np
from jax import lax
from jax.experimental import pallas as pl
from jax.experimental.pallas import tpu as pltpu
from jax.sharding import PartitionSpec as P

MESH = pl.DeviceIdType.MESH
F32 = jnp.float32
BF16 = jnp.bfloat16
I32 = jnp.int32
PAYOFF_UNIT = 1.0 / 4096.0
VMEM = pltpu.VMEM
LEAVES = 64
SIDES = 4


def dot(a, b):
    return jnp.dot(a, b, preferred_element_type=F32)


def dot_t(a, b):
    return lax.dot_general(a, b, (((1,), (1,)), ((), ())), preferred_element_type=F32)


def lane_take(table, lanes):
    return jnp.take_along_axis(table, lanes, axis=1, mode="promise_in_bounds")


def look_up(first, second, index):
    lanes = index & 127
    tile = index >> 7
    parts = []
    for m in range(8):
        parts.append(jnp.where(tile == m, lane_take(first[m], lanes), 0.0))
        parts.append(jnp.where(tile == m + 8, lane_take(second[m], lanes), 0.0))
    while len(parts) > 1:
        parts = [parts[i] + parts[i + 1] for i in range(0, len(parts), 2)]
    return parts[0]


def card_hits(card, low, high):
    return (card == low) | (card == high)


def kernel(
    br_act,
    up_ref,
    root_ref,
    parent_ref,
    opp_ref,
    br_ref,
    cards_ref,
    board_ref,
    rank_ref,
    opp_act_ref,
    kind_ref,
    stake_ref,
    w_hbm,
    level_ref,
    value_ref,
    best_ref,
    w_ref,
    apart,
    s1,
    r1,
    s2,
    r2,
    s3,
    r3,
    s4,
    r4,
    sy,
    ry,
    sy_scale,
    ry_scale,
    relay,
    sx,
    rx,
    br_all,
    weights,
    now_ref,
    turned,
    board_sum,
    reach_ref,
    inverse,
    packed,
    value_rows,
    level_rank,
    column,
    wide_rank,
    code_turn,
    code_rows,
    board_turn,
    board_col,
    node_ref,
    compat_all,
    sub_ref,
    left,
    right,
    right_up,
    leaf_send,
    leaf_recv,
    own_sem,
    w_sem,
    near_send,
    near_recv,
    near_scale_send,
    near_scale_recv,
    relay_send,
    relay_recv,
    far_send,
    far_recv,
    far_scale_send,
    far_scale_recv,
    x_send,
    x_recv,
    b_send,
    b_recv,
):
    leaf_at = lax.axis_index("leaf")
    hand_at = lax.axis_index("hand")
    barrier = pltpu.get_barrier_semaphore()

    plane, place = leaf_at // 8, lax.rem(leaf_at, 8)
    along = [lax.rem(place + step, 8) for step in (4, 5, 3, 2, 6, 7, 1, 0)]

    def each_leaf(do):
        def one_plane(turn, carry):
            half, odd = (turn + 1) // 2, lax.rem(turn, 2)
            start = lax.rem(plane + 4 + half - 2 * half * odd, 8) * 8
            for step in along:
                do(start + step)
            return carry

        lax.fori_loop(0, 7, one_plane, 0)
        for step in along[:7]:
            do(plane * 8 + step)

    def greet_leaf(peer):
        pl.semaphore_signal(barrier, inc=1, device_id={"leaf": peer}, device_id_type=MESH)

    each_leaf(greet_leaf)
    for i in range(1, SIDES):
        pl.semaphore_signal(
            barrier, inc=1, device_id={"hand": lax.rem(hand_at + i, SIDES)}, device_id_type=MESH
        )
    w_copy = pltpu.make_async_copy(w_hbm, w_ref, w_sem)
    w_copy.start()

    def leaf_start(number, src, dst):
        own = pltpu.make_async_copy(src.at[leaf_at], dst.at[leaf_at], own_sem.at[number])
        own.start()

        def send(peer):
            pltpu.make_async_remote_copy(
                src_ref=src.at[peer],
                dst_ref=dst.at[leaf_at],
                send_sem=leaf_send.at[number],
                recv_sem=leaf_recv.at[number],
                device_id={"leaf": peer},
                device_id_type=MESH,
            ).start()

        each_leaf(send)
        return own

    def leaf_wait(number, own, src, dst):
        own.wait()
        others = pl.ds(0, LEAVES - 1)
        pltpu.make_async_copy(dst.at[others], dst.at[others], leaf_recv.at[number]).wait()
        pltpu.make_async_copy(src.at[others], src.at[others], leaf_send.at[number]).wait()

    root_row = jnp.concatenate([root_ref[...], jnp.full((1, 32), 2048, I32)], axis=1)
    whole_a = (up_ref[:, 0:128].astype(F32) * 512.0).T.astype(I32)
    whole_b = (up_ref[:, 128:256].astype(F32) * 512.0).T.astype(I32)
    packed[...] = (whole_a << 16) | whole_b
    for d in range(LEAVES):
        s1[d, 0:2, :] = packed[2 * d : 2 * d + 2, :]
        s1[d, 2:3, :] = root_row

    low_r, high_r = cards_ref[0:1, :], cards_ref[1:2, :]
    lane64 = lax.broadcasted_iota(I32, (8, 128), 1)
    code_turn[64:128, :] = jnp.zeros((64, 128), F32)
    action = lax.broadcasted_iota(I32, (8, 96), 0)
    for a in range(8):
        allowed = action < opp_act_ref[a : a + 1, :]
        stake = stake_ref[a].astype(F32)
        stake = jnp.where(kind_ref[a] == 1, 0.0 - stake, stake)
        code_turn[a * 8 : a * 8 + 8, 0:96] = jnp.where(allowed, stake, 0.0)
    code_rows[...] = code_turn[...].T
    board_turn[0:5, 0:96] = board_ref[...].astype(F32)
    board_col[...] = board_turn[...].T
    for g in range(3):
        rows = pl.ds(pl.multiple_of(hand_at * 24 + g * 8, 8), 8)
        hit = jnp.zeros((8, 1024), F32)
        for c in range(5):
            card = jnp.broadcast_to(board_col[rows, c : c + 1], (8, 1024))
            hit = jnp.where(card_hits(card, low_r, high_r), 1.0, hit)
        compat_all[g * 8 : g * 8 + 8, :] = (1.0 - hit) * PAYOFF_UNIT
    mine = pl.ds(pl.multiple_of(hand_at * 256, 256), 256)
    low_m, high_m = cards_ref[0:1, mine], cards_ref[1:2, mine]
    for g in range(12):
        hit = jnp.zeros((8, 256), F32)
        for c in range(5):
            card = jnp.broadcast_to(board_col[g * 8 : g * 8 + 8, c : c + 1], (8, 256))
            hit = jnp.where(card_hits(card, low_m, high_m), 1.0, hit)
        board_sum[g * 8 : g * 8 + 8, :] = (1.0 - hit) * opp_ref[...]
    lane_row = lax.broadcasted_iota(I32, (128, 128), 0)
    for k in range(3):
        for t in range(16):
            index = parent_ref[k : k + 1, t * 128 : t * 128 + 128] & 127
            right_up[k, :, t * 128 : t * 128 + 128] = jnp.where(
                jnp.broadcast_to(index, (128, 128)) == lane_row, 1.0, 0.0
            ).astype(BF16)

    def clear(s, carry):
        node_ref[s] = jnp.zeros((8, 1024), F32)
        return carry

    lax.fori_loop(0, 24, clear, 0)

    for g in range(3):
        rows = pl.ds(pl.multiple_of(hand_at * 24 + g * 8, 8), 8)
        rank = rank_ref[rows, :]
        spread = ((rank & 127) + 128).astype(F32)
        power = rank >> 7
        for bit in range(6):
            spread = spread * jnp.where((power >> bit) & 1 == 1, float(2 ** (2**bit)), 1.0)
        level_rank[g * 8 : g * 8 + 8, :] = spread
        for m in range(8):
            column[g, m * 128 : m * 128 + 128, 0:8] = spread[:, m * 128 : m * 128 + 128].T
    pl.semaphore_wait(barrier, LEAVES - 1 + SIDES - 1)
    own1 = leaf_start(0, s1, r1)
    br_copies = []
    for i in range(1, SIDES):
        peer = lax.rem(hand_at + i, SIDES)
        copy = pltpu.make_async_remote_copy(
            src_ref=br_ref,
            dst_ref=br_all.at[hand_at],
            send_sem=b_send.at[i],
            recv_sem=b_recv.at[i],
            device_id={"hand": peer},
            device_id_type=MESH,
        )
        copy.start()
        br_copies.append(copy)
    br_all[hand_at] = br_ref[...]

    card_row = lax.broadcasted_iota(I32, (128, 1024), 0).astype(F32)
    holds = jnp.where(card_hits(card_row, low_r, high_r), 1.0, 0.0)
    holds_narrow = holds.astype(BF16)
    for j in range(8):
        shared = dot(holds[:, j * 128 : j * 128 + 128].T.astype(BF16), holds_narrow)
        keep = jnp.maximum(1.0 - shared, 0.0)
        for k in range(8):
            for m in range(8):
                tile = keep[k * 16 : k * 16 + 16, m * 128 : m * 128 + 128].astype(BF16)
                apart[j * 8 + k, m, 0] = tile
                apart[j * 8 + k, m, 1] = -tile

    def widen(j, carry):
        g, t = j // 4, lax.rem(j, 4) * 16
        for k in range(8):
            for i in range(16):
                rows = pl.ds(pl.multiple_of((t + i) * 16, 16), 16)
                wide_rank[g * 8 + k, t + i] = jnp.broadcast_to(
                    column[g, rows, k : k + 1], (16, 128)
                ).astype(BF16)
        return carry

    lax.fori_loop(0, 12, widen, 0)

    leaf_wait(0, own1, s1, r1)

    low_half = lax.broadcasted_iota(I32, (8, 128), 0) < 4
    place8 = lax.broadcasted_iota(I32, (8, 128), 1) // 32
    for m in range(8):
        pairs = []
        for q in range(4):
            one, two = r1[4 * m + q, 0:2, :], r1[32 + 4 * m + q, 0:2, :]
            four = jnp.concatenate([one >> 16, one & 65535, two >> 16, two & 65535], axis=0)
            pairs.append(four.astype(F32) * (1.0 / 512.0))
        for level in range(4):
            out = jnp.zeros((8, 128), F32)
            for q in range(4):
                shift = ((q - level) * 32) % 128
                moved = pairs[q] if shift == 0 else pltpu.roll(pairs[q], shift, 1)
                out = jnp.where(place8 == q, moved, out)
            if level == 0:
                now_ref[:, m * 128 : m * 128 + 128] = out
            else:
                weights[level - 1, :, m * 128 : m * 128 + 128] = out

    def tables():
        first, second = [], []
        for m in range(8):
            here = now_ref[:, m * 128 : (m + 1) * 128]
            swapped = pltpu.roll(here, 4, 0)
            first.append(jnp.where(low_half, here, swapped))
            second.append(jnp.where(low_half, swapped, here))
        return first, second

    def wide_row(a, b):
        return jnp.where(low_half, jnp.broadcast_to(a, (8, 128)), jnp.broadcast_to(b, (8, 128)))

    for level in range(3):
        first, second = tables()
        for m in range(8):
            cut = slice(m * 128, (m + 1) * 128)
            index = wide_row(
                parent_ref[level : level + 1, m * 128 : m * 128 + 128],
                parent_ref[level : level + 1, 1024 + m * 128 : 1024 + m * 128 + 128],
            )
            now_ref[:, cut] = look_up(first, second, index) * weights[level, :, cut]
    first, second = tables()

    def reach_of(j, carry):
        for k in range(4):
            i = j * 4 + k
            index = wide_row(r1[2 * i, 2:3, :], r1[2 * i + 1, 2:3, :])
            out = look_up(first, second, index)
            s2[2 * i] = out[0:4]
            s2[2 * i + 1] = out[4:8]
        return carry

    lax.fori_loop(0, 8, reach_of, 0)
    own2 = leaf_start(1, s2, r2)

    w_copy.wait()
    own_block = (lane64 // 8 == lax.broadcasted_iota(I32, (8, 128), 0)) & (lane64 < 64)

    def spread_code(s):
        code = jnp.broadcast_to(code_rows[pl.ds(s, 1), :], (8, 128))
        return jnp.where(own_block, code, 0.0)[:, 0:64]

    def totals(i, carry):
        for k in range(8):
            s = i * 8 + k
            legal = jnp.where(spread_code(s) == 0.0, 0.0, 1.0).astype(BF16)
            inverse[s] = 1.0 / dot(legal, w_ref[s])
        return carry

    lax.fori_loop(0, 12, totals, 0)

    def target(j, carry):
        for k in range(2):
            i = j * 2 + k
            index = r1[i, 2:3, :] & 127
            right[i] = jnp.where(
                jnp.broadcast_to(index, (128, 128)) == lane_row, 1.0, 0.0
            ).astype(BF16)
        return carry

    lax.fori_loop(0, LEAVES // 2, target, 0)

    leaf_wait(1, own2, s2, r2)

    for d in range(LEAVES):
        turned[2 * d : 2 * d + 2, :] = r2[d, 0:2, :]
        turned[128 + 2 * d : 130 + 2 * d, :] = r2[d, 2:4, :]
    for half in range(2):
        cut = slice(half * 128, half * 128 + 128)
        reach_ref[:, cut] = turned[cut, :].T[0:96, :] * board_sum[0:96, cut]

    def leaf_group(owner, g, dst, dst_scale):
        scales = jnp.zeros((8, 128), F32)
        for k in range(8):
            s = owner * 24 + g * 8 + k
            code = spread_code(s)
            stake = jnp.abs(code)
            high = jnp.floor(stake * 0.0625) * 16.0
            low = stake - high
            shown = code < 0.0
            coef = jnp.concatenate(
                [
                    jnp.where(shown, high, 0.0),
                    jnp.where(shown, low, 0.0),
                    jnp.where(shown, 0.0, high),
                    jnp.where(shown, 0.0, low),
                ],
                axis=0,
            ).astype(BF16)
            factor = reach_ref[pl.ds(s, 1), :] * inverse[s]
            wide = w_ref[s].astype(F32).reshape(8, 8, 256) * factor[:, None, :]
            y = dot(coef, wide.reshape(64, 256).astype(BF16))
            y1 = y[0:8] + y[8:16]
            y0 = y[16:24] + y[24:32]
            top1 = jnp.max(y1, axis=1, keepdims=True)
            top0 = jnp.max(y0, axis=1, keepdims=True)
            whole1 = jnp.floor(y1 * (32767.0 / jnp.maximum(top1, 1e-30)) + 0.5).astype(I32)
            whole0 = jnp.floor(y0 * (65535.0 / jnp.maximum(top0, 1e-30)) + 0.5).astype(I32)
            dst[g * 8 + k] = (whole1 << 16) | whole0
            scales = jnp.where(lane64 == 2 * k, top1 * (1.0 / 32767.0), scales)
            scales = jnp.where(lane64 == 2 * k + 1, top0 * (1.0 / 65535.0), scales)
        dst_scale[g] = scales

    def unit(q, g):
        first_strip = q * 16
        ranks = level_rank[pl.ds(pl.multiple_of(g * 8, 8), 8), :]
        shown_rows, fold_rows = [], []
        for s in range(8):
            both = ry[q, g * 8 + s]
            shown_y, fold_y = both >> 16, both & 65535
            for whole, rows in ((shown_y, shown_rows), (fold_y, fold_rows)):
                small = whole & 255
                rows.append(
                    jnp.concatenate([(whole - small).astype(F32), small.astype(F32)], axis=0).astype(BF16)
                )
        lows = jnp.concatenate(fold_rows, axis=0)
        scales = ry_scale[q, g]

        for n in range(4):
            cut = slice(n * 256, n * 256 + 256)
            fold = dot(
                lows,
                jnp.concatenate(
                    [
                        jnp.concatenate(
                            [apart[first_strip + part, m, 0] for part in range(16)], axis=0
                        )
                        for m in (2 * n, 2 * n + 1)
                    ],
                    axis=1,
                ),
            )
            for s in range(8):
                sides = []
                for m in (2 * n, 2 * n + 1):
                    row = jnp.broadcast_to(
                        ranks[s : s + 1, m * 128 : m * 128 + 128], (16, 128)
                    ).astype(BF16)
                    strips = []
                    for part in range(16):
                        at = first_strip + part
                        gap = row - wide_rank[g * 8 + s, at]
                        strips.append(jnp.maximum(jnp.minimum(gap, apart[at, m, 0]), apart[at, m, 1]))
                    sides.append(jnp.concatenate(strips, axis=0))
                total = dot(shown_rows[s], jnp.concatenate(sides, axis=1))
                node = (total[0:8] + total[8:16]) * scales[:, 2 * s : 2 * s + 1]
                node = node + (
                    fold[s * 16 : s * 16 + 8] + fold[s * 16 + 8 : s * 16 + 16]
                ) * scales[:, 2 * s + 1 : 2 * s + 2]
                node_ref[g * 8 + s, :, cut] = node_ref[g * 8 + s, :, cut] + node

    across = lax.rem(hand_at + 2, SIDES)
    beside = (lax.rem(hand_at + 1, SIDES), lax.rem(hand_at + 3, SIDES))
    halves = (pl.ds(0, 12), pl.ds(12, 12))

    def to_hand(peer, src, dst, send_sem, recv_sem):
        return pltpu.make_async_remote_copy(
            src_ref=src,
            dst_ref=dst,
            send_sem=send_sem,
            recv_sem=recv_sem,
            device_id={"hand": peer},
            device_id_type=MESH,
        )

    def leaf_across(g, carry):
        leaf_group(across, g, sy.at[across], sy_scale.at[across])
        return carry

    lax.fori_loop(0, 3, leaf_across, 0)
    relays = [
        to_hand(beside[i], sy.at[across, halves[i]], relay.at[i], relay_send.at[i], relay_recv.at[i])
        for i in range(2)
    ]
    for copy in relays:
        copy.start()
    far_scale = to_hand(
        across, sy_scale.at[across], ry_scale.at[hand_at], far_scale_send, far_scale_recv
    )
    far_scale.start()

    def near_copies(i, g):
        peer = beside[i]
        rows = pl.ds(pl.multiple_of(g * 8, 8), 8)
        return (
            to_hand(
                peer, sy.at[peer, rows], ry.at[hand_at, rows], near_send.at[i, g], near_recv.at[i, g]
            ),
            to_hand(
                peer,
                sy_scale.at[peer, g],
                ry_scale.at[hand_at, g],
                near_scale_send.at[i, g],
                near_scale_recv.at[i, g],
            ),
        )

    def leaf_near(g, carry):
        for i in range(2):
            leaf_group(beside[i], g, sy.at[beside[i]], sy_scale.at[beside[i]])
            for copy in near_copies(i, g):
                copy.start()
        return carry

    lax.fori_loop(0, 3, leaf_near, 0)

    def leaf_own(g, carry):
        leaf_group(hand_at, g, ry.at[hand_at], ry_scale.at[hand_at])
        return carry

    lax.fori_loop(0, 3, leaf_own, 0)

    def unit_own(g, carry):
        unit(hand_at, g)
        return carry

    lax.fori_loop(0, 3, unit_own, 0)
    fars = []
    for i in range(2):
        relays[i].wait_recv()
        far = to_hand(
            beside[i], relay.at[i], ry.at[beside[1 - i], halves[i]], far_send.at[i], far_recv.at[i]
        )
        far.start()
        fars.append(far)

    def unit_near(j, carry):
        g, i = j // 2, lax.rem(j, 2)
        for copy in near_copies_any(i, g):
            copy.wait_recv()
        unit(lax.rem(hand_at + 3 - 2 * i, SIDES), g)
        return carry

    def near_copies_any(i, g):
        peer = lax.rem(hand_at + 1 + 2 * i, SIDES)
        rows = pl.ds(pl.multiple_of(g * 8, 8), 8)
        return (
            to_hand(
                peer, sy.at[peer, rows], ry.at[hand_at, rows], near_send.at[i, g], near_recv.at[i, g]
            ),
            to_hand(
                peer,
                sy_scale.at[peer, g],
                ry_scale.at[hand_at, g],
                near_scale_send.at[i, g],
                near_scale_recv.at[i, g],
            ),
        )

    lax.fori_loop(0, 6, unit_near, 0)
    for far in fars:
        far.wait_recv()
    far_scale.wait_recv()

    def unit_across(g, carry):
        unit(across, g)
        return carry

    lax.fori_loop(0, 3, unit_across, 0)

    def near_done(j, carry):
        for copy in near_copies_any(lax.rem(j, 2), j // 2):
            copy.wait_send()
        return carry

    lax.fori_loop(0, 6, near_done, 0)
    for i in range(2):
        relays[i].wait_send()
        fars[i].wait_send()
    far_scale.wait_send()
    for copy in br_copies:
        copy.wait()

    act_row = lax.broadcasted_iota(I32, (8, 1024), 0)

    def best_of(g, carry):
        for k in range(8):
            s = g * 8 + k
            value = node_ref[s] * compat_all[pl.ds(s, 1), :]
            value = jnp.where(act_row < br_act[hand_at * 24 + s], value, -1e30)
            sub_ref[pl.ds(s, 1), :] = jnp.max(value, axis=0, keepdims=True)
        return carry

    lax.fori_loop(0, 3, best_of, 0)
    board_total = jnp.sum(sub_ref[...], axis=0, keepdims=True)
    weighted = jnp.zeros((1, 256), F32)
    range_sum = jnp.zeros((1, 256), F32)
    for p in range(SIDES):
        weighted += board_total[:, p * 256 : p * 256 + 256] * br_all[p]
        range_sum += br_all[p]
    for p in range(SIDES):
        sx[p, 0:24, :] = sub_ref[:, p * 256 : p * 256 + 256]
        sx[p, 24:25, :] = weighted
    rx[hand_at] = sx[hand_at]
    x_copies = []
    for i in (2, 1, 3):
        peer = lax.rem(hand_at + i, SIDES)
        copy = pltpu.make_async_remote_copy(
            src_ref=sx.at[peer],
            dst_ref=rx.at[hand_at],
            send_sem=x_send.at[i],
            recv_sem=x_recv.at[i],
            device_id={"hand": peer},
            device_id_type=MESH,
        )
        copy.start()
        x_copies.append(copy)
    for copy in x_copies:
        copy.wait()

    for p in range(SIDES):
        board_sum[p * 24 : p * 24 + 24, :] = rx[p, 0:24, :]
    sides = (rx[0, 24:25, :] + rx[1, 24:25, :]) + (rx[2, 24:25, :] + rx[3, 24:25, :])
    side = jnp.sum(sides[:, 0:128] + sides[:, 128:256], axis=1, keepdims=True)
    board_sum[96:128, :] = jnp.broadcast_to(side, (32, 256))
    for half in range(2):
        cut = slice(half * 128, half * 128 + 128)
        turned[cut, :] = board_sum[:, cut].T
    for d in range(LEAVES):
        s3[d, 0:2, :] = turned[2 * d : 2 * d + 2, :]
        s3[d, 2:4, :] = turned[128 + 2 * d : 130 + 2 * d, :]
    own3 = leaf_start(2, s3, r3)
    leaf_wait(2, own3, s3, r3)

    upper = lax.broadcasted_iota(I32, (8, 128), 0) // 4

    def choose(values, index, put):
        twice = jnp.concatenate([values, values], axis=0)
        high = twice.astype(BF16).astype(F32)
        low = twice - high
        big = jnp.broadcast_to(index >> 7, (8, 128))
        for i in range(4):
            is_a, is_b = big == 4 * i + upper, big == 4 * i + 2 + upper
            put(
                i * 16,
                jnp.concatenate(
                    [jnp.where(is_a, high, 0.0), jnp.where(is_b, high, 0.0)], axis=0
                ).astype(BF16),
            )
            put(
                64 + i * 16,
                jnp.concatenate(
                    [jnp.where(is_a, low, 0.0), jnp.where(is_b, low, 0.0)], axis=0
                ).astype(BF16),
            )

    def from_boards(j, carry):
        for k in range(4):
            i = j * 4 + k

            def put(row, block):
                left[i, row : row + 16, :] = block

            choose(r3[i], r1[i, 2:3, :], put)
        return carry

    lax.fori_loop(0, 16, from_boards, 0)
    acc = jnp.zeros((128, 128), F32)
    for i in range(0, LEAVES, 2):
        acc = acc + dot_t(
            jnp.concatenate([left[i], left[i + 1]], axis=1),
            jnp.concatenate([right[i], right[i + 1]], axis=1),
        )
    levels = [None] * 4
    levels[3] = acc[0:64] + acc[64:128]
    for level in range(2, -1, -1):
        for t in range(16):

            def put(row, block, t=t):
                left[t, row : row + 16, :] = block

            choose(
                levels[level + 1][4 * t : 4 * t + 4],
                parent_ref[level : level + 1, t * 128 : t * 128 + 128],
                put,
            )
        acc = jnp.zeros((128, 128), F32)
        for t in range(0, 16, 2):
            acc = acc + dot_t(
                jnp.concatenate([left[t], left[t + 1]], axis=1),
                right_up[level, :, t * 128 : t * 128 + 256],
            )
        levels[level] = acc[0:64] + acc[64:128]

    column_sum = jnp.zeros((8, 128), F32)
    for t in range(8):
        column_sum = column_sum + levels[0][8 * t : 8 * t + 8]
    column_sum = column_sum[0:4] + column_sum[4:8]
    root4 = jnp.sum(column_sum, axis=1, keepdims=True) * (1.0 / 2048.0)
    lane4 = lax.broadcasted_iota(I32, (4, 128), 1)
    at4 = (lane4 & 3) == lax.broadcasted_iota(I32, (4, 128), 0)
    value_row = jnp.sum(jnp.where(at4, root4, 0.0), axis=0, keepdims=True)
    place64 = lax.broadcasted_iota(I32, (64, 128), 1) // 32
    for q in range(4):
        out = jnp.zeros((64, 128), F32)
        for level in range(4):
            shift = ((level - q) * 32) % 128
            moved = levels[level] if shift == 0 else pltpu.roll(levels[level], shift, 1)
            out = jnp.where(place64 == level, moved, out)
        for t in range(16):
            s4[4 * t + q, 0:4, :] = out[4 * t : 4 * t + 4]
            s4[4 * t + q, 4:5, :] = value_row
    own4 = leaf_start(3, s4, r4)
    best_sum = jnp.zeros((1, 128), F32)
    for d in range(LEAVES):
        best_sum = best_sum + r3[d, 0:1, :]
    numerator = best_sum[:, 96:97] * (1.0 / 2048.0)
    denominator = jnp.sum(range_sum, axis=1, keepdims=True)
    best_ref[...] = numerator / denominator
    leaf_wait(3, own4, s4, r4)
    for d in range(LEAVES):
        turned[2 * d : 2 * d + 2, :] = r4[d, 0:2, :]
        turned[128 + 2 * d : 130 + 2 * d, :] = r4[d, 2:4, :]
        value_rows[d : d + 1, :] = r4[d, 4:5, :]
    source = lax.broadcasted_iota(I32, (8, 128), 0)
    value_a = jnp.zeros((8, 128), F32)
    value_b = jnp.zeros((8, 128), F32)
    for t in range(8):
        rows = value_rows[8 * t : 8 * t + 8, :]
        is_own = lane64 >> 1 == source + 8 * t
        value_a = value_a + jnp.where(is_own, lane_take(rows, lane64 & 1), 0.0)
        value_b = value_b + jnp.where(is_own, lane_take(rows, (lane64 & 1) + 2), 0.0)
    value_ref[:, 0:128] = jnp.sum(value_a, axis=0, keepdims=True)
    value_ref[:, 128:256] = jnp.sum(value_b, axis=0, keepdims=True)
    for half in range(2):
        cut = slice(half * 128, half * 128 + 128)
        level_ref[:, cut] = turned[cut, :].T


def write_kernel(a_ref, b_ref, c_ref, a_out, b_out, c_out):
    a_out[...] = a_ref[...]
    b_out[...] = b_ref[...]
    c_out[...] = c_ref[...]


def hand_cards(number):
    low_list = []
    high_list = []
    for low_card in range(52):
        for high_card in range(low_card + 1, 52):
            low_list.append(low_card)
            high_list.append(high_card)
    chosen = np.arange(number) * 1326 // number
    return np.stack([np.array(low_list)[chosen], np.array(high_list)[chosen]]).astype(np.int32)


def local(
    opp_range,
    br_range,
    up_weight,
    up_parent,
    board_cards,
    hand_rank,
    root_parent,
    br_actions,
    opp_actions,
    leaf_kind,
    leaf_stake,
    opp_weight,
):
    cards = hand_cards(1024).astype(np.float32)
    vmem = pl.BlockSpec(memory_space=VMEM)
    sem = pltpu.SemaphoreType.DMA
    level_out, root_value, best = pl.pallas_call(
        kernel,
        out_shape=(
            jax.ShapeDtypeStruct((128, 256), F32),
            jax.ShapeDtypeStruct((1, 256), F32),
            jax.ShapeDtypeStruct((1, 1), F32),
        ),
        in_specs=[pl.BlockSpec(memory_space=pltpu.SMEM)]
        + [vmem] * 11
        + [pl.BlockSpec(memory_space=pl.ANY)],
        out_specs=(vmem, vmem, vmem),
        scratch_shapes=[
            VMEM((96, 64, 256), BF16),
            VMEM((64, 8, 2, 16, 128), BF16),
            VMEM((LEAVES, 3, 128), I32),
            VMEM((LEAVES, 3, 128), I32),
            VMEM((LEAVES, 4, 128), F32),
            VMEM((LEAVES, 4, 128), F32),
            VMEM((LEAVES, 4, 128), F32),
            VMEM((LEAVES, 4, 128), F32),
            VMEM((LEAVES, 5, 128), F32),
            VMEM((LEAVES, 5, 128), F32),
            VMEM((SIDES, 24, 8, 256), I32),
            VMEM((SIDES, 24, 8, 256), I32),
            VMEM((SIDES, 3, 8, 128), F32),
            VMEM((SIDES, 3, 8, 128), F32),
            VMEM((2, 12, 8, 256), I32),
            VMEM((SIDES, 25, 256), F32),
            VMEM((SIDES, 25, 256), F32),
            VMEM((SIDES, 1, 256), F32),
            VMEM((3, 8, 1024), F32),
            VMEM((8, 1024), F32),
            VMEM((256, 128), F32),
            VMEM((128, 256), F32),
            VMEM((96, 256), F32),
            VMEM((96, 8, 256), F32),
            VMEM((128, 128), I32),
            VMEM((LEAVES, 128), F32),
            VMEM((24, 1024), F32),
            VMEM((3, 1024, 8), F32),
            VMEM((24, 64, 16, 128), BF16),
            VMEM((128, 128), F32),
            VMEM((128, 128), F32),
            VMEM((8, 128), F32),
            VMEM((128, 8), F32),
            VMEM((24, 8, 1024), F32),
            VMEM((24, 1024), F32),
            VMEM((24, 1024), F32),
            VMEM((LEAVES, 128, 128), BF16),
            VMEM((LEAVES, 128, 128), BF16),
            VMEM((3, 128, 2048), BF16),
            sem((4,)),
            sem((4,)),
            sem((4,)),
            sem,
            sem((2, 3)),
            sem((2, 3)),
            sem((2, 3)),
            sem((2, 3)),
            sem((2,)),
            sem((2,)),
            sem((2,)),
            sem((2,)),
            sem,
            sem,
            sem((4,)),
            sem((4,)),
            sem((4,)),
            sem((4,)),
        ],
        compiler_params=pltpu.CompilerParams(collective_id=0, has_side_effects=True),
        name="tree",
    )(
        br_actions,
        up_weight.reshape(128, 256),
        root_parent.reshape(1, 96),
        up_parent,
        opp_range.reshape(1, 256),
        br_range.reshape(1, 256),
        jnp.asarray(cards),
        board_cards.T,
        hand_rank,
        opp_actions.T,
        leaf_kind.transpose(1, 2, 0),
        leaf_stake.transpose(1, 2, 0),
        opp_weight.reshape(96, 64, 256),
    )
    level_out, root_value, best = pl.pallas_call(
        write_kernel,
        out_shape=(
            jax.ShapeDtypeStruct((128, 256), F32),
            jax.ShapeDtypeStruct((1, 256), F32),
            jax.ShapeDtypeStruct((1, 1), F32),
        ),
        name="write",
    )(level_out, root_value, best)
    return level_out.reshape(4, 32, 256), root_value.reshape(256), best[0, 0]


def solution(mesh):
    in_specs = (
        P("hand"),
        P("hand"),
        P(None, "leaf", "hand"),
        P(),
        P("leaf", None),
        P("leaf", None),
        P("leaf"),
        P("leaf"),
        P("leaf", None),
        P("leaf", None, None),
        P("leaf", None, None),
        P("leaf", None, None, "hand"),
    )
    out_specs = (P(None, "leaf", "hand"), P("hand"), P())
    return jax.shard_map(local, mesh=mesh, in_specs=in_specs, out_specs=out_specs, check_vma=False)
```
